8 devices in a mesh: dp: 1 (over z), tp: 2 (over y), ep: 4 (over x, core).
Axes of the slice: x: 2, y: 2, z: 1, core: 2. Of those that a mesh axis runs over, the one named last changes fastest.
Arguments:
- x: bfloat16 [128, 512, 768], P(('dp', 'ep'))
- src_len: int32 [128], P(('dp', 'ep'))
- expert_idx: int32 [128, 512, 2], P(('dp', 'ep'))
- ln_gain: float32 [4, 768], replicated
- ln_bias: float32 [4, 768], replicated
- w_query: bfloat16 [2, 768, 12, 64], P(None, None, 'tp')
- b_query: float32 [2, 12, 64], P(None, 'tp')
- w_key: bfloat16 [2, 768, 12, 64], P(None, None, 'tp')
- w_value: bfloat16 [2, 768, 12, 64], P(None, None, 'tp')
- b_value: float32 [2, 12, 64], P(None, 'tp')
- w_attn_out: bfloat16 [2, 12, 64, 768], P(None, 'tp')
- b_attn_out: float32 [2, 768], replicated
- w_fc1: bfloat16 [768, 3072], P(None, 'tp')
- b_fc1: float32 [3072], P('tp')
- w_fc2: bfloat16 [3072, 768], P('tp')
- b_fc2: float32 [768], replicated
- w_router: float32 [768, 16], replicated
- w_exp_in: bfloat16 [16, 768, 3072], P('ep', None, 'tp')
- b_exp_in: float32 [16, 3072], P('ep', 'tp')
- w_exp_out: bfloat16 [16, 3072, 768], P('ep', 'tp')
- b_exp_out: float32 [16, 768], P('ep')
Outputs:
- output: bfloat16 [128, 512, 768], P(('dp', 'ep'))
All inputs are finite; a program needn't handle non-finite values.
Results may differ from the reference program's by a relative error of at most 0.0135335.
Values are sent between devices in bfloat16 or wider.
A program may use at most 1 GiB of HBM per device.

```python
import jax
import jax.numpy as jnp
from jax import lax

GROUPS = 4
ROWS_DEV = 32
SEQ_LEN = 512
D_MODEL = 768
NUM_HEADS = 12
HEAD_DIM = 64
FF_DENSE = 3072
EXPERTS = 16
EXPERT_FF = 3072

BATCH = GROUPS * ROWS_DEV
TOKENS_GROUP = ROWS_DEV * SEQ_LEN
CAPACITY = 2 * ((TOKENS_GROUP + EXPERTS - 1) // EXPERTS)
DUMP_SLOT = EXPERTS * CAPACITY
INNER_DIM = NUM_HEADS * HEAD_DIM
LN_EPS = 1e-5


def layer_norm(hidden, gain, shift):
    hidden = hidden.astype(jnp.float32)
    centered = hidden - jnp.mean(hidden, axis=-1, keepdims=True)
    variance = jnp.mean(centered * centered, axis=-1, keepdims=True)
    return centered * lax.rsqrt(variance + LN_EPS) * gain + shift


def draw_routing(route_key):
    len_key, hot_key, pick_key, first_key, second_key = jax.random.split(route_key, 5)
    row_ids = jnp.arange(BATCH)
    lengths = jax.random.randint(len_key, (BATCH,), SEQ_LEN // 4, SEQ_LEN + 1)
    lengths = jnp.where(row_ids == 0, SEQ_LEN, lengths)
    lengths = jnp.where(row_ids == BATCH - 1, SEQ_LEN // 4, lengths)
    hot_count = max(EXPERTS // 16, 1)
    hot_start = jax.random.randint(hot_key, (), 0, EXPERTS)
    grid = (BATCH, SEQ_LEN)
    pick_hot = jax.random.randint(pick_key, grid, 0, 4) == 0
    uniform_first = jax.random.randint(first_key, grid, 0, EXPERTS)
    hot_first = (hot_start + uniform_first % hot_count) % EXPERTS
    first = jnp.where(pick_hot, hot_first, uniform_first)
    second = (first + jax.random.randint(second_key, grid, 1, EXPERTS)) % EXPERTS
    expert_idx = jnp.stack([first, second], axis=-1).astype(jnp.int32)
    return lengths.astype(jnp.int32), expert_idx


def scaled_normal(key, extent, scale):
    return jax.random.normal(key, extent, jnp.float32) * scale


def setup_inputs(seed: int = 0, part: int = 0) -> dict:
    part_key = jax.random.fold_in(jax.random.key(seed), part)
    x_key, route_key = jax.random.split(part_key, 2)
    keys = jax.random.split(jax.random.key(seed + 1), 18)
    src_len, expert_idx = draw_routing(route_key)
    attn_shape = (2, D_MODEL, NUM_HEADS, HEAD_DIM)
    model_scale = D_MODEL ** -0.5
    inner_scale = INNER_DIM ** -0.5
    return {
        'x': scaled_normal(x_key, (BATCH, SEQ_LEN, D_MODEL), 1.0).astype(jnp.bfloat16),
        'src_len': src_len,
        'expert_idx': expert_idx,
        'ln_gain': 1.0 + scaled_normal(keys[0], (4, D_MODEL), 0.2),
        'ln_bias': scaled_normal(keys[1], (4, D_MODEL), 0.2),
        'w_query': scaled_normal(keys[2], attn_shape, model_scale).astype(jnp.bfloat16),
        'b_query': scaled_normal(keys[3], (2, NUM_HEADS, HEAD_DIM), 0.5),
        'w_key': scaled_normal(keys[4], attn_shape, model_scale).astype(jnp.bfloat16),
        'w_value': scaled_normal(keys[5], attn_shape, model_scale).astype(jnp.bfloat16),
        'b_value': scaled_normal(keys[6], (2, NUM_HEADS, HEAD_DIM), 0.5),
        'w_attn_out': scaled_normal(keys[7], (2, NUM_HEADS, HEAD_DIM, D_MODEL), inner_scale).astype(jnp.bfloat16),
        'b_attn_out': scaled_normal(keys[8], (2, D_MODEL), 0.3),
        'w_fc1': scaled_normal(keys[9], (D_MODEL, FF_DENSE), model_scale).astype(jnp.bfloat16),
        'b_fc1': scaled_normal(keys[10], (FF_DENSE,), 0.5),
        'w_fc2': scaled_normal(keys[11], (FF_DENSE, D_MODEL), FF_DENSE ** -0.5).astype(jnp.bfloat16),
        'b_fc2': scaled_normal(keys[12], (D_MODEL,), 0.3),
        'w_router': scaled_normal(keys[13], (D_MODEL, EXPERTS), model_scale),
        'w_exp_in': scaled_normal(keys[14], (EXPERTS, D_MODEL, EXPERT_FF), model_scale).astype(jnp.bfloat16),
        'b_exp_in': scaled_normal(keys[15], (EXPERTS, EXPERT_FF), 0.5),
        'w_exp_out': scaled_normal(keys[16], (EXPERTS, EXPERT_FF, D_MODEL), EXPERT_FF ** -0.5).astype(jnp.bfloat16),
        'b_exp_out': scaled_normal(keys[17], (EXPERTS, D_MODEL), 0.5),
    }


def attention_row(residual, key_ok, gain, shift, w_q, b_q, w_k, w_v, b_v, w_o, b_o):
    normed = layer_norm(residual, gain, shift).astype(jnp.bfloat16)

    def project(weight):
        flat = jnp.dot(normed, weight.reshape(D_MODEL, INNER_DIM), preferred_element_type=jnp.float32)
        return flat.reshape(SEQ_LEN, NUM_HEADS, HEAD_DIM)

    query = (project(w_q) + b_q).astype(jnp.bfloat16)
    keys = project(w_k).astype(jnp.bfloat16)
    values = (project(w_v) + b_v).astype(jnp.bfloat16)
    scores = jnp.einsum('qhk,shk->hqs', query.astype(jnp.float32), keys.astype(jnp.float32)) * (HEAD_DIM ** -0.5)
    scores = jnp.where(key_ok[None, None, :], scores, -1e30)
    attn_probs = jax.nn.softmax(scores, axis=-1).astype(jnp.bfloat16)
    context = jnp.einsum('hqs,shk->qhk', attn_probs.astype(jnp.float32), values.astype(jnp.float32)).astype(jnp.bfloat16)
    projected = jnp.dot(context.reshape(SEQ_LEN, INNER_DIM), w_o.reshape(INNER_DIM, D_MODEL), preferred_element_type=jnp.float32)
    return (residual.astype(jnp.float32) + projected + b_o).astype(jnp.bfloat16)


def dense_ffn(residual, gain, shift, w_in, b_in, w_out, b_out):
    normed = layer_norm(residual, gain, shift).astype(jnp.bfloat16)
    inner = jax.nn.relu(jnp.dot(normed, w_in, preferred_element_type=jnp.float32) + b_in).astype(jnp.bfloat16)
    projected = jnp.dot(inner, w_out, preferred_element_type=jnp.float32)
    return (residual.astype(jnp.float32) + projected + b_out).astype(jnp.bfloat16)


def take_rows(rows, index):
    return rows[index]


def fill_table(dest_first, dest_second):
    token_ids = jnp.arange(TOKENS_GROUP, dtype=jnp.int32)
    table = jnp.full((DUMP_SLOT + 1,), TOKENS_GROUP, jnp.int32)
    table = table.at[dest_first].set(token_ids).at[dest_second].set(token_ids)
    return table[:DUMP_SLOT]


def run_expert(operands):
    rows_in, w_in, b_in, w_out, b_out = operands
    inner = jax.nn.relu(jnp.dot(rows_in, w_in, preferred_element_type=jnp.float32) + b_in).astype(jnp.bfloat16)
    return (jnp.dot(inner, w_out, preferred_element_type=jnp.float32) + b_out).astype(jnp.bfloat16)


def reference(x, src_len, expert_idx, ln_gain, ln_bias, w_query, b_query, w_key, w_value, b_value, w_attn_out, b_attn_out, w_fc1, b_fc1, w_fc2, b_fc2, w_router, w_exp_in, b_exp_in, w_exp_out, b_exp_out):
    positions = jnp.arange(SEQ_LEN)

    def row_layers(row_pair):
        row, length = row_pair
        key_ok = positions < length
        hidden = attention_row(row, key_ok, ln_gain[0], ln_bias[0], w_query[0], b_query[0], w_key[0], w_value[0], b_value[0], w_attn_out[0], b_attn_out[0])
        hidden = dense_ffn(hidden, ln_gain[1], ln_bias[1], w_fc1, b_fc1, w_fc2, b_fc2)
        hidden = attention_row(hidden, key_ok, ln_gain[2], ln_bias[2], w_query[1], b_query[1], w_key[1], w_value[1], b_value[1], w_attn_out[1], b_attn_out[1])
        normed = layer_norm(hidden, ln_gain[3], ln_bias[3])
        logits = jnp.dot(normed, w_router, preferred_element_type=jnp.float32)
        return hidden, normed.astype(jnp.bfloat16), logits

    residual, normed, logits = lax.map(row_layers, (x, src_len))
    grouped = (GROUPS, TOKENS_GROUP)
    valid = (positions[None, :] < src_len[:, None]).reshape(grouped)
    first = expert_idx[..., 0].reshape(grouped)
    second = expert_idx[..., 1].reshape(grouped)
    router_probs = jax.nn.softmax(logits, axis=-1).reshape(GROUPS, TOKENS_GROUP, EXPERTS)
    prob_first = jnp.take_along_axis(router_probs, first[..., None], axis=-1)[..., 0]
    prob_second = jnp.take_along_axis(router_probs, second[..., None], axis=-1)[..., 0]
    gate_first = prob_first / (prob_first + prob_second)
    gate_second = prob_second / (prob_first + prob_second)
    expert_ids = jnp.arange(EXPERTS)
    hot_first = ((first[..., None] == expert_ids) & valid[..., None]).astype(jnp.int32)
    hot_second = ((second[..., None] == expert_ids) & valid[..., None]).astype(jnp.int32)
    rank_first = jnp.cumsum(hot_first, axis=1) - 1
    rank_second = jnp.cumsum(hot_second, axis=1) - 1 + jnp.sum(hot_first, axis=1, keepdims=True)
    slot_first = jnp.sum(rank_first * hot_first, axis=-1)
    slot_second = jnp.sum(rank_second * hot_second, axis=-1)
    dest_first = jnp.where(valid & (slot_first < CAPACITY), first * CAPACITY + slot_first, DUMP_SLOT)
    dest_second = jnp.where(valid & (slot_second < CAPACITY), second * CAPACITY + slot_second, DUMP_SLOT)
    tables = jax.vmap(fill_table)(dest_first, dest_second)
    zero_row = jnp.zeros((GROUPS, 1, D_MODEL), jnp.bfloat16)
    padded = jnp.concatenate([normed.reshape(GROUPS, TOKENS_GROUP, D_MODEL), zero_row], axis=1)
    dispatched = jax.vmap(take_rows)(padded, tables)
    per_expert = dispatched.reshape(GROUPS, EXPERTS, CAPACITY, D_MODEL).transpose(1, 0, 2, 3).reshape(EXPERTS, GROUPS * CAPACITY, D_MODEL)
    expert_out = lax.map(run_expert, (per_expert, w_exp_in, b_exp_in, w_exp_out, b_exp_out))
    returned = expert_out.reshape(EXPERTS, GROUPS, CAPACITY, D_MODEL).transpose(1, 0, 2, 3).reshape(GROUPS, DUMP_SLOT, D_MODEL)
    returned = jnp.concatenate([returned, zero_row], axis=1)
    out_first = jax.vmap(take_rows)(returned, dest_first).astype(jnp.float32)
    out_second = jax.vmap(take_rows)(returned, dest_second).astype(jnp.float32)
    combined = gate_first[..., None] * out_first + gate_second[..., None] * out_second
    result = residual.reshape(GROUPS, TOKENS_GROUP, D_MODEL).astype(jnp.float32) + combined
    return result.astype(jnp.bfloat16).reshape(BATCH, SEQ_LEN, D_MODEL)
```

```python
import functools

import jax
import jax.numpy as jnp
from jax import lax
from jax.experimental import pallas as pl
from jax.experimental.pallas import tpu as pltpu
from jax.sharding import PartitionSpec as P

LN_EPS = 1e-5
TILE_ROWS = 256
CHUNKS = 4
SECTION_SIZES = (3072, 3584)


def layer_norm(hidden, gain, shift):
    hidden = hidden.astype(jnp.float32)
    centered = hidden - jnp.mean(hidden, axis=-1, keepdims=True)
    variance = jnp.mean(centered * centered, axis=-1, keepdims=True)
    return centered * lax.rsqrt(variance + LN_EPS) * gain + shift


def attention_layer(residual, key_ok, gain, shift, w_q, b_q, w_k, w_v, b_v, w_o, b_o):
    normed = layer_norm(residual, gain, shift).astype(jnp.bfloat16)
    query = (jnp.einsum('rsd,tdhk->rsthk', normed, w_q, preferred_element_type=jnp.float32) + b_q).astype(jnp.bfloat16)
    keys = jnp.einsum('rsd,tdhk->rsthk', normed, w_k, preferred_element_type=jnp.float32).astype(jnp.bfloat16)
    values = (jnp.einsum('rsd,tdhk->rsthk', normed, w_v, preferred_element_type=jnp.float32) + b_v).astype(jnp.bfloat16)
    scores = jnp.einsum('rqthk,rsthk->rthqs', query, keys, preferred_element_type=jnp.float32) * (w_q.shape[-1] ** -0.5)
    scores = jnp.where(key_ok[:, None, None, None, :], scores, -1e30)
    attn_probs = jax.nn.softmax(scores, axis=-1).astype(jnp.bfloat16)
    context = jnp.einsum('rthqs,rsthk->rqthk', attn_probs, values, preferred_element_type=jnp.float32).astype(jnp.bfloat16)
    total = jnp.einsum('rqthk,thkd->rqd', context, w_o, preferred_element_type=jnp.float32)
    return (residual.astype(jnp.float32) + total + b_o).astype(jnp.bfloat16)


def dense_ffn(residual, gain, shift, w_in, b_in, w_out, b_out):
    normed = layer_norm(residual, gain, shift).astype(jnp.bfloat16)
    inner = jax.nn.relu(jnp.einsum('rsd,tdf->rstf', normed, w_in, preferred_element_type=jnp.float32) + b_in).astype(jnp.bfloat16)
    total = jnp.einsum('rstf,tfd->rsd', inner, w_out, preferred_element_type=jnp.float32)
    return (residual.astype(jnp.float32) + total + b_out).astype(jnp.bfloat16)


def expert_kernel(visit_tile, visit_expert, visit_lo, visit_hi, n_visits, x_ref, w_in, b_in, w_out, b_out, o_ref):
    step = pl.program_id(0)

    @pl.when(step < n_visits[0])
    def _():
        rows = x_ref[...]
        total = b_out[0]
        for part in range(w_in.shape[0]):
            inner = jnp.dot(rows, w_in[part, 0], preferred_element_type=jnp.float32) + b_in[part, 0]
            inner = jnp.maximum(inner, 0.0).astype(jnp.bfloat16)
            total = total + jnp.dot(inner, w_out[part, 0], preferred_element_type=jnp.float32)
        row = lax.broadcasted_iota(jnp.int32, total.shape, 0)
        inside = (row >= visit_lo[step]) & (row < visit_hi[step])
        o_ref[...] = jnp.where(inside, total, o_ref[...].astype(jnp.float32)).astype(jnp.bfloat16)


def plan_visits(counts, max_visits):
    ends = jnp.cumsum(counts)
    starts = ends - counts
    tiles = jnp.where(counts > 0, (ends - 1) // TILE_ROWS - starts // TILE_ROWS + 1, 0)
    visit_ends = jnp.cumsum(tiles)
    n_visits = visit_ends[-1:]
    step = jnp.minimum(jnp.arange(max_visits, dtype=jnp.int32), jnp.maximum(n_visits - 1, 0))
    expert = jnp.minimum(jnp.sum(step[:, None] >= visit_ends[None, :], axis=1), counts.shape[0] - 1).astype(jnp.int32)
    hot = expert[:, None] == jnp.arange(counts.shape[0], dtype=jnp.int32)

    def pick(values):
        return jnp.sum(jnp.where(hot, values, 0), axis=1)

    tile = pick(starts // TILE_ROWS - (visit_ends - tiles)) + step
    base = tile * TILE_ROWS
    return tile, expert, pick(starts) - base, pick(ends) - base, n_visits


def expert_ffn(rows, plan, w_in, b_in, w_out, b_out):
    count, d_model = rows.shape
    parts, local_experts, _, hidden = w_in.shape
    visits = count // TILE_ROWS + local_experts

    def row_map(i, tile, expert, lo, hi, n):
        return (tile[i], 0)

    def weight_map(i, tile, expert, lo, hi, n):
        return (0, expert[i], 0, 0)

    return pl.pallas_call(
        expert_kernel,
        grid_spec=pltpu.PrefetchScalarGridSpec(
            num_scalar_prefetch=5,
            grid=(visits,),
            in_specs=[
                pl.BlockSpec((TILE_ROWS, d_model), row_map),
                pl.BlockSpec((parts, 1, d_model, hidden), weight_map),
                pl.BlockSpec((parts, 1, 1, hidden), weight_map),
                pl.BlockSpec((parts, 1, hidden, d_model), weight_map),
                pl.BlockSpec((1, 1, d_model), lambda i, tile, expert, lo, hi, n: (expert[i], 0, 0)),
            ],
            out_specs=pl.BlockSpec((TILE_ROWS, d_model), row_map),
        ),
        out_shape=jax.ShapeDtypeStruct((count, d_model), jnp.bfloat16),
        compiler_params=pltpu.CompilerParams(dimension_semantics=('arbitrary',)),
        cost_estimate=pl.CostEstimate(flops=4 * count * d_model * hidden * parts, bytes_accessed=4 * count * d_model, transcendentals=0),
    )(*plan, rows, w_in, b_in[:, :, None, :], w_out, b_out[:, None, :])


def exclusive_sum(values, axis=0):
    return jnp.cumsum(values, axis=axis) - values


def solution(mesh):
    ep_size = mesh.shape['ep']
    tp_size = mesh.shape['tp']

    def local_fn(x, src_len, expert_idx, ln_gain, ln_bias, w_query, b_query, w_key, w_value, b_value, w_attn_out, b_attn_out, w_fc1, b_fc1, w_fc2, b_fc2, w_router, w_exp_in, b_exp_in, w_exp_out, b_exp_out):
        rows, seq_len, d_model = x.shape
        tokens = rows * seq_len
        num_experts = w_router.shape[1]
        capacity = 2 * (-(-tokens // num_experts))
        local_experts = w_exp_in.shape[0]
        half_rows = rows // tp_size
        half = half_rows * seq_len
        me_t = lax.axis_index('tp')
        me_e = lax.axis_index('ep')

        gather = functools.partial(lax.all_gather, axis_name='tp', axis=0, tiled=False)
        small = jnp.concatenate([v.reshape(-1) for v in (b_query, b_value, b_fc1, b_exp_in)])
        small = gather(small)
        cuts = [0]
        for v in (b_query, b_value, b_fc1, b_exp_in):
            cuts.append(cuts[-1] + v.size)
        full_b_query, full_b_value, full_b_fc1, full_b_exp_in = [
            small[:, lo:hi].reshape((tp_size,) + v.shape)
            for v, lo, hi in zip((b_query, b_value, b_fc1, b_exp_in), cuts[:-1], cuts[1:])]
        heads = w_query.shape[2]
        head_dim = w_query.shape[3]
        inner_dim = heads * head_dim

        def gather_attention(j):
            packed = jnp.stack([w[j].reshape(d_model, inner_dim) for w in (w_query, w_key, w_value)] + [w_attn_out[j].reshape(inner_dim, d_model).reshape(d_model, inner_dim)])
            whole = gather(packed)
            w_q, w_k, w_v = [whole[:, i].reshape(tp_size, d_model, heads, head_dim) for i in range(3)]
            return w_q, w_k, w_v, whole[:, 3].reshape(tp_size, inner_dim, d_model).reshape(tp_size, heads, head_dim, d_model)

        attn0 = gather_attention(0)
        full_fc1 = gather(w_fc1)
        full_fc2 = gather(w_fc2)
        attn1 = gather_attention(1)
        full_exp_in = gather(w_exp_in)
        full_exp_out = gather(w_exp_out)

        def mine(array):
            return lax.dynamic_index_in_dim(array.reshape((half_rows, tp_size) + array.shape[1:]), me_t, 1, keepdims=False)

        key_ok_all = jnp.arange(seq_len)[None, :] < src_len[:, None]
        expert_ids = jnp.arange(num_experts, dtype=jnp.int32)
        valid = key_ok_all.reshape(tokens)
        first = expert_idx[..., 0].reshape(tokens)
        second = expert_idx[..., 1].reshape(tokens)
        hot_first = ((first[:, None] == expert_ids) & valid[:, None]).astype(jnp.int32)
        hot_second = ((second[:, None] == expert_ids) & valid[:, None]).astype(jnp.int32)
        sum_first = jnp.cumsum(hot_first, axis=0)
        sum_second = jnp.cumsum(hot_second, axis=0) + sum_first[-1]
        kept_first = jnp.where(sum_first <= capacity, hot_first, 0).reshape(rows, seq_len, num_experts)
        kept_second = jnp.where(sum_second <= capacity, hot_second, 0).reshape(rows, seq_len, num_experts)
        part_first = jnp.sum(kept_first.reshape(half_rows, tp_size, seq_len, num_experts), axis=(0, 2))
        part_second = jnp.sum(kept_second.reshape(half_rows, tp_size, seq_len, num_experts), axis=(0, 2))
        all_counts = lax.all_gather(part_first + part_second, 'ep')
        most = jnp.max(jnp.sum(all_counts.reshape(ep_size, tp_size, ep_size, local_experts), axis=3))
        my_counts = lax.dynamic_index_in_dim(part_first + part_second, me_t, 0, keepdims=False).reshape(ep_size, local_experts)
        my_counts_first = lax.dynamic_index_in_dim(part_first, me_t, 0, keepdims=False)
        offsets = exclusive_sum(my_counts, axis=1).reshape(num_experts)
        my_first = mine(kept_first).reshape(half, num_experts)
        my_second = mine(kept_second).reshape(half, num_experts)
        pos_first = jnp.sum((jnp.cumsum(my_first, axis=0) - 1 + offsets) * my_first, axis=1)
        pos_second = jnp.sum((jnp.cumsum(my_second, axis=0) - 1 + offsets + my_counts_first) * my_second, axis=1)
        keep_first = jnp.sum(my_first, axis=1) > 0
        keep_second = jnp.sum(my_second, axis=1) > 0
        choice_first = mine(expert_idx[..., 0]).reshape(half)
        choice_second = mine(expert_idx[..., 1]).reshape(half)
        dest_first = (choice_first // local_experts) ^ me_e
        dest_second = (choice_second // local_experts) ^ me_e
        most_rows = half
        token_ids = jnp.arange(half, dtype=jnp.int32)
        dump = ep_size * most_rows
        table = jnp.zeros((dump,), jnp.int32).at[jnp.concatenate([
            jnp.where(keep_first, dest_first * most_rows + pos_first, dump),
            jnp.where(keep_second, dest_second * most_rows + pos_second, dump),
        ])].set(jnp.concatenate([token_ids, token_ids]), mode='drop').reshape(ep_size, most_rows)
        swap = {s: [(i, i ^ s) for i in range(ep_size)] for s in range(1, ep_size)}
        tables = [table[0]] + [lax.ppermute(table[s], 'ep', swap[s]) for s in range(1, ep_size)]
        section_counts = lax.dynamic_index_in_dim(lax.dynamic_index_in_dim(all_counts, me_t, 1, keepdims=False).reshape(ep_size, ep_size, local_experts), me_e, 1, keepdims=False)
        max_visits = most_rows // TILE_ROWS + local_experts
        plans = [plan_visits(lax.dynamic_index_in_dim(section_counts, me_e ^ s, 0, keepdims=False), max_visits) for s in range(ep_size)]

        x_half = mine(x)
        key_ok = mine(key_ok_all)
        chunk = half_rows // CHUNKS
        hidden_parts, logit_parts = [], []
        sections = [[] for _ in range(ep_size)]
        for c in range(CHUNKS):
            part = slice(c * chunk, (c + 1) * chunk)
            hidden = attention_layer(x_half[part], key_ok[part], ln_gain[0], ln_bias[0], attn0[0], full_b_query[:, 0], attn0[1], attn0[2], full_b_value[:, 0], attn0[3], b_attn_out[0])
            hidden = dense_ffn(hidden, ln_gain[1], ln_bias[1], full_fc1, full_b_fc1.reshape(tp_size, -1), full_fc2, b_fc2)
            hidden = attention_layer(hidden, key_ok[part], ln_gain[2], ln_bias[2], attn1[0], full_b_query[:, 1], attn1[1], attn1[2], full_b_value[:, 1], attn1[3], b_attn_out[1])
            normed_f32 = layer_norm(hidden, ln_gain[3], ln_bias[3]).reshape(chunk * seq_len, d_model)
            logit_parts.append(jnp.dot(normed_f32, w_router, preferred_element_type=jnp.float32))
            hidden_parts.append(hidden.reshape(chunk * seq_len, d_model))
            sent = normed_f32.astype(jnp.bfloat16)
            across = lax.ppermute(sent, 'ep', swap[2])
            sections[0].append(sent)
            sections[1].append(lax.ppermute(sent, 'ep', swap[1]))
            sections[2].append(across)
            sections[3].append(lax.ppermute(across, 'ep', swap[1]))

        logits = jnp.concatenate(logit_parts, axis=0)
        logit_first = jnp.sum(jnp.where(choice_first[:, None] == expert_ids, logits, 0.0), axis=1)
        logit_second = jnp.sum(jnp.where(choice_second[:, None] == expert_ids, logits, 0.0), axis=1)
        gate_first = jnp.where(keep_first, jax.nn.sigmoid(logit_first - logit_second), 0.0)
        gate_second = jnp.where(keep_second, jax.nn.sigmoid(logit_second - logit_first), 0.0)
        section_rows = [jnp.concatenate(parts, axis=0) for parts in sections]

        def experts(size):
            def run():
                back = [None] * ep_size
                for s in (3, 2, 1, 0):
                    rows_in = section_rows[s][tables[s][:size]]
                    out = expert_ffn(rows_in, plans[s], full_exp_in, full_b_exp_in, full_exp_out, b_exp_out)
                    back[s] = lax.ppermute(out, 'ep', swap[s]) if s else out
                flat = jnp.concatenate(back, axis=0)
                rows_first = flat[jnp.where(keep_first, dest_first * size + pos_first, 0)].astype(jnp.float32)
                rows_second = flat[jnp.where(keep_second, dest_second * size + pos_second, 0)].astype(jnp.float32)
                combined = jnp.where(keep_first[:, None], gate_first[:, None] * rows_first, 0.0) + jnp.where(keep_second[:, None], gate_second[:, None] * rows_second, 0.0)
                return (jnp.concatenate(hidden_parts, axis=0).astype(jnp.float32) + combined).astype(jnp.bfloat16)
            return run

        sizes = [size for size in SECTION_SIZES if size < most_rows] + [most_rows]
        level = sum((most > size).astype(jnp.int32) for size in sizes[:-1])
        result = lax.switch(level, [experts(size) for size in sizes])
        return lax.all_gather(result.reshape(half_rows, 1, seq_len, d_model), 'tp', axis=1, tiled=True).reshape(rows, seq_len, d_model)

    in_specs = (P(('dp', 'ep'), None, None), P(('dp', 'ep')), P(('dp', 'ep'), None, None), P(), P(), P(None, None, 'tp', None), P(None, 'tp', None), P(None, None, 'tp', None), P(None, None, 'tp', None), P(None, 'tp', None), P(None, 'tp', None, None), P(), P(None, 'tp'), P('tp'), P('tp', None), P(), P(), P('ep', None, 'tp'), P('ep', 'tp'), P('ep', 'tp', None), P('ep', None))
    return jax.shard_map(local_fn, mesh=mesh, in_specs=in_specs, out_specs=P(('dp', 'ep'), None, None), check_vma=False)
```
